256 devices in a mesh: grp: 8 (over x, core), dp: 32 (over z, y).
Axes of the slice: x: 4, y: 4, z: 8, core: 2. Of those that a mesh axis runs over, the one named last changes fastest.
Arguments:
- gradients: bfloat16 [8, 32, 16384, 128], P('grp', 'dp'), may hold values from -48 to 48
- block_len: int32 [16], replicated, may hold values from 1 to 524288, 2097152 in all
- amax_history: float32 [4, 16], replicated, may hold values from 20 to 200
Outputs:
- mean_grad: bfloat16 [16384, 128], P('dp')
- block_amax: bfloat16 [16], replicated
The draws below stay inside these ranges and needn't reach their ends.
Inputs may be any that keep to these rules, and one draw needn't show every extreme that they name: `block_len`: every tensor has at least one entry; the lengths sum to 2097152.
All inputs are finite; a program needn't handle non-finite values.
Results may differ from the reference program's by a relative error of at most 0.018.
Values may be sent and summed in bfloat16 or wider, within the bound.
No kernel may reach another device: no remote copies, remote signals or barrier semaphores. Data moves between devices by JAX's collectives and lax.ppermute only.
A program may use at most 64 MiB of HBM per device.

```python
import math
import jax
import jax.numpy as jnp
import numpy as np
from jax import lax

ROWS = 16384
BLOCKS = 16
HIST = 4
N_GRP = 8
N_DP = 32
DEVICES = 256


def block_scale(own_key, dims, cuts, least, largest):
    factor_of = 1.0
    for dim, shards_of in cuts:
        draws = jax.random.uniform(jax.random.fold_in(jax.random.fold_in(own_key, 6), dim), (shards_of,), jnp.float32, least / len(cuts), largest / len(cuts))
        factor_of = factor_of * jnp.repeat(jnp.exp(draws), dims[dim] // shards_of).reshape((-1,) + (1,) * (len(dims) - 1 - dim))
    return factor_of


def split_up(count, total, most, lean):
    weights = [(1 << 20) // math.isqrt(rank ** lean) + 1 for rank in range(2, count + 1)]
    surplus, counts = total - most - (count - 1), [1] * (count - 1)
    while surplus > 0:
        candidates = [i for i in range(count - 1) if counts[i] < most]
        mass, budget = sum([weights[i] for i in candidates]), surplus
        for i in candidates:
            extra = min(most - counts[i], max(1, budget * weights[i] // mass), surplus)
            counts[i] = counts[i] + extra
            surplus = surplus - extra
    return np.array([most] + counts)


def uneven(own_key, amount, total, bound, skew):
    if amount == 2:
        one = jax.random.randint(own_key, (), max(1, total - bound), min(bound, total - 1) + 1)
        return jnp.stack([one, total - one])
    lengths = jnp.asarray(split_up(amount, total, bound, skew), jnp.int32)
    couples = (amount - 1) // 2
    giver, sink = lengths[1:1 + 2 * couples:2], lengths[2:2 + 2 * couples:2]
    slack = jnp.minimum(giver - 1, bound - sink)
    passed = jax.random.randint(jax.random.fold_in(own_key, 1), (couples,), 0, 1 << 20) % (slack + 1)
    lengths = lengths.at[1:1 + 2 * couples:2].set(giver - passed).at[2:2 + 2 * couples:2].set(sink + passed)
    return lengths[jax.random.permutation(jax.random.fold_in(own_key, 2), amount)]


def noise(rng, extent, spread, most, shards=(), held_as=jnp.bfloat16):
    entries = spread * jax.random.normal(rng, extent, jnp.float32)
    if shards:
        entries = entries * block_scale(rng, extent, shards, -0.22, 0.18)
    return jnp.clip(entries, -most, most).astype(held_as)


def setup_inputs(seed: int = 0) -> dict:
    key_list = jax.random.split(jax.random.key(seed), 4)
    return {
        "gradients": noise(key_list[0], (N_GRP, N_DP, ROWS, 128), 8.0, 48.0, ((0, 8), (1, 32))),
        "block_len": uneven(key_list[1], BLOCKS, ROWS * 128, ROWS * 32, 2).astype(jnp.int32),
        "amax_history": jnp.clip(jnp.exp(jax.random.uniform(key_list[2], (HIST, BLOCKS), jnp.float32, math.log(20.0), math.log(200.0))), 20.0, 200.0),
    }


SATURATE = 448.0


def reference(gradients, block_len, amax_history):
    block_ends = jnp.cumsum(block_len).astype(jnp.int32)
    position = (jnp.arange(ROWS, dtype=jnp.int32)[:, None] * 128 + jnp.arange(128, dtype=jnp.int32)[None, :])
    block = jnp.sum((position[:, :, None] >= block_ends[None, None, :]).astype(jnp.int32), axis=-1)
    in_block = block[:, :, None] == jnp.arange(BLOCKS, dtype=jnp.int32)[None, None, :]
    scales = SATURATE / jnp.maximum(jnp.max(amax_history, axis=0), 1.0)
    scale_elem = jnp.sum(jnp.where(in_block, scales[None, None, :], jnp.float32(0.0)), axis=-1)

    def one_group(carry, group_grads):
        accumulated, maxima = carry
        summed = jnp.sum(group_grads.astype(jnp.float32), axis=0)
        local_max = jnp.max(jnp.where(in_block, jnp.abs(summed)[:, :, None], jnp.float32(0.0)), axis=(0, 1))
        quantized = jnp.clip(summed * scale_elem, -SATURATE, SATURATE).astype(jnp.bfloat16)
        return (accumulated + quantized.astype(jnp.float32), jnp.maximum(maxima, local_max)), None

    start = (jnp.zeros((ROWS, 128), jnp.float32), jnp.zeros((BLOCKS,), jnp.float32))
    (accumulated, maxima), unused = lax.scan(one_group, start, gradients)
    mean_grad = (accumulated / scale_elem / DEVICES).astype(jnp.bfloat16)
    return mean_grad, maxima.astype(jnp.bfloat16)
```

```python
import jax
import jax.numpy as jnp
from jax import lax
from jax.experimental import pallas as pl
from jax.experimental.pallas import tpu as pltpu
from jax.sharding import Mesh
from jax.sharding import PartitionSpec as P

SATURATE = 448.0
SIZE = {"x": 4, "c": 2, "z": 8, "y": 4}
ROWS = 512
A = 272
B = ROWS - A
BLOCKS = 16
DEVICES = 256


def shift(x, axis, by):
    n = SIZE[axis]
    return lax.ppermute(x, axis, [(i, (i + by) % n) for i in range(n)])


def f32(x):
    return x.astype(jnp.float32)


def add(*terms):
    total = f32(terms[0])
    for t in terms[1:]:
        total = total + f32(t)
    return total


def bf(x):
    return x.astype(jnp.bfloat16)


def prepare_kernel(at_ref, len_ref, hist_ref, block_ref, scale_ref):
    position = (
        at_ref[0] * (ROWS * 128)
        + lax.broadcasted_iota(jnp.int32, (ROWS, 128), 0) * 128
        + lax.broadcasted_iota(jnp.int32, (ROWS, 128), 1)
    )
    largest = jnp.maximum(jnp.max(hist_ref[...], axis=0, keepdims=True), 1.0)
    scales = SATURATE / largest
    block = jnp.zeros((ROWS, 128), jnp.int32)
    scale = jnp.broadcast_to(scales[:, 0:1], (ROWS, 128))
    end = jnp.int32(0)
    for c in range(1, BLOCKS):
        end = end + len_ref[c - 1]
        past = position >= end
        block = jnp.where(past, c, block)
        scale = jnp.where(past, scales[:, c : c + 1], scale)
    block_ref[...] = block
    scale_ref[...] = scale


def prepare(at, block_len, amax_history):
    return pl.pallas_call(
        prepare_kernel,
        out_shape=(
            jax.ShapeDtypeStruct((ROWS, 128), jnp.int32),
            jax.ShapeDtypeStruct((ROWS, 128), jnp.float32),
        ),
        in_specs=[
            pl.BlockSpec(memory_space=pltpu.SMEM),
            pl.BlockSpec(memory_space=pltpu.SMEM),
            pl.BlockSpec(memory_space=pltpu.VMEM),
        ],
        out_specs=[pl.BlockSpec(memory_space=pltpu.VMEM)] * 2,
        name="prepare",
    )(at, block_len, amax_history)


def quantize_kernel(sa_ref, sb_ref, block_ref, scale_ref, q_ref, m_ref):
    for ref, lo, n in ((sa_ref, 0, A), (sb_ref, A, B)):
        q = jnp.clip(ref[...] * scale_ref[lo : lo + n], -SATURATE, SATURATE)
        q_ref[lo : lo + n] = q.astype(jnp.bfloat16)
    for c in range(BLOCKS):
        top = jnp.zeros((8, 128), jnp.float32)
        for ref, lo, n in ((sa_ref, 0, A), (sb_ref, A, B)):
            own = jnp.where(block_ref[lo : lo + n] == c, jnp.abs(ref[...]), 0.0)
            top = jnp.maximum(top, jnp.max(own.reshape(n // 8, 8, 128), axis=0))
        m_ref[c : c + 1] = jnp.max(top, axis=0, keepdims=True)


def quantize(sa, sb, block, scale):
    return pl.pallas_call(
        quantize_kernel,
        out_shape=(
            jax.ShapeDtypeStruct((ROWS, 128), jnp.bfloat16),
            jax.ShapeDtypeStruct((BLOCKS, 128), jnp.float32),
        ),
        in_specs=[pl.BlockSpec(memory_space=pltpu.VMEM)] * 4,
        out_specs=[pl.BlockSpec(memory_space=pltpu.VMEM)] * 2,
        name="quantize",
    )(sa, sb, block, scale)


def body(gradients, block_len, amax_history):
    g = gradients.reshape(8, 4, ROWS, 128)
    z, y = lax.axis_index("z"), lax.axis_index("y")

    def for_y(dy, z0, nz):
        at = (jnp.int32(z0), (y + dy) % 4, jnp.int32(0), jnp.int32(0))
        return lax.dynamic_slice(g, at, (nz, 1, A, 128)).reshape(nz, A, 128)

    def for_z(dz, y0, ny):
        at = ((z + dz) % 8, jnp.int32(y0), jnp.int32(A), jnp.int32(0))
        return lax.dynamic_slice(g, at, (1, ny, B, 128)).reshape(ny, B, 128)

    a_up = shift(for_y(2, 0, 4), "y", 1)
    a_dn = shift(for_y(2, 4, 4), "y", -1)
    b_up = shift(for_z(4, 0, 2), "z", 1)
    b_dn = shift(for_z(4, 2, 2), "z", -1)

    a_up = shift(jnp.concatenate([bf(add(for_y(1, 0, 4), a_up)), for_y(1, 4, 4)]), "y", 1)
    a_dn = shift(jnp.concatenate([for_y(-1, 0, 4), bf(add(for_y(-1, 4, 4), a_dn))]), "y", -1)

    b_up = shift(jnp.concatenate([bf(add(for_z(3, 0, 2), b_up)), for_z(3, 2, 2)]), "z", 1)
    b_dn = shift(jnp.concatenate([for_z(-3, 0, 2), bf(add(for_z(-3, 2, 2), b_dn))]), "z", -1)
    b_up = shift(bf(add(for_z(2, 0, 4), b_up)), "z", 1)
    b_dn = shift(bf(add(for_z(-2, 0, 4), b_dn)), "z", -1)

    pa = bf(add(for_y(0, 0, 8), a_up, a_dn))

    def chunk(dz):
        return lax.dynamic_slice_in_dim(pa, (z + dz) % 8, 1, 0)

    a_dn = shift(jnp.concatenate([chunk(-2), chunk(-4)]), "z", -1)
    a_up = shift(jnp.concatenate([chunk(1), chunk(3)]), "z", 1)
    a_one = shift(bf(add(chunk(-1), a_dn[0:1])), "z", -1)
    a_three = shift(bf(add(chunk(-3), a_dn[1:2])), "z", -3)
    a_two = shift(bf(add(chunk(2), a_up[1:2])), "z", 2)
    sa = add(chunk(0), a_up[0:1], a_one, a_three, a_two)[0]

    b_up = shift(bf(add(for_z(1, 0, 4), b_up)), "z", 1)
    b_dn = shift(bf(add(for_z(-1, 0, 4), b_dn)), "z", -1)
    pb = bf(add(for_z(0, 0, 4), b_up, b_dn))

    def piece(dy):
        return lax.dynamic_slice_in_dim(pb, (y + dy) % 4, 1, 0)

    sb = add(piece(0), shift(piece(1), "y", 1), shift(piece(-1), "y", -1), shift(piece(2), "y", 2))[0]

    at = (z * 4 + y).reshape(1).astype(jnp.int32)
    block, scale = prepare(at, block_len, amax_history)
    q, m = quantize(sa, sb, block, scale)

    both = add(q, shift(q, "x", 2))
    sides = add(shift(q, "x", 1), shift(q, "x", -1))
    chips = both + sides
    accumulated = chips + shift(chips, "c", 1)
    mean_grad = bf(accumulated / scale / DEVICES)

    m = bf(m)
    for axis, hops in (("z", (1, -1)), ("z", (3, -3)), ("y", (1, -1, 2)), ("x", (1, -1, 2)), ("c", (1,))):
        seen = [m] + [shift(m, axis, by) for by in hops]
        m = seen[0]
        for s in seen[1:]:
            m = jnp.maximum(m, s)
    return mean_grad, jnp.max(m, axis=1)


def solution(mesh):
    torus = Mesh(mesh.devices.reshape(4, 2, 8, 4), ("x", "c", "z", "y"))
    placed = (P(("x", "c"), ("z", "y"), None, None), P(), P())
    return jax.shard_map(
        body, mesh=torus, in_specs=placed, out_specs=(P(("z", "y"), None), P()), check_vma=False
    )
```

```python
import jax
import jax.numpy as jnp
from jax import lax
from jax.experimental import pallas as pl
from jax.experimental.pallas import tpu as pltpu
from jax.sharding import Mesh
from jax.sharding import PartitionSpec as P


SATURATE = 448.0
SIZE = {"x": 4, "c": 2, "z": 8, "y": 4}
ROWS = 512
A = 256
B = ROWS - A
BLOCKS = 16
DEVICES = 256


def shift(x, axis, by):
    n = SIZE[axis]
    return lax.ppermute(x, axis, [(i, (i + by) % n) for i in range(n)])


def f32(x):
    return x.astype(jnp.float32)


def add(*terms):
    total = f32(terms[0])
    for t in terms[1:]:
        total = total + f32(t)
    return total


def bf(x):
    return x.astype(jnp.bfloat16)


def together(*arrays):
    return lax.optimization_barrier(arrays)


def swap(x, axis, by):
    return lax.ppermute(x, axis, [(i, i ^ by) for i in range(SIZE[axis])])


def in_vmem(x):
    return pltpu.with_memory_space_constraint(x, pltpu.VMEM)


VMEM = pl.BlockSpec(memory_space=pltpu.VMEM)
SMEM = pl.BlockSpec(memory_space=pltpu.SMEM)


def prepare_kernel(at_ref, len_ref, hist_ref, block_ref, scale_ref):
    position = (
        (at_ref[0] * 4 + at_ref[1]) * (ROWS * 128)
        + lax.broadcasted_iota(jnp.int32, (ROWS, 128), 0) * 128
        + lax.broadcasted_iota(jnp.int32, (ROWS, 128), 1)
    )
    largest = jnp.maximum(jnp.max(hist_ref[...], axis=0, keepdims=True), 1.0)
    scales = SATURATE / largest
    block = jnp.zeros((ROWS, 128), jnp.int32)
    scale = jnp.broadcast_to(scales[:, 0:1], (ROWS, 128))
    end = jnp.int32(0)
    for c in range(1, BLOCKS):
        end = end + len_ref[c - 1]
        past = position >= end
        block = jnp.where(past, c, block)
        scale = jnp.where(past, scales[:, c : c + 1], scale)
    block_ref[...] = block
    scale_ref[...] = scale


def prepare(at, block_len, amax_history):
    return pl.pallas_call(
        prepare_kernel,
        out_shape=(
            jax.ShapeDtypeStruct((ROWS, 128), jnp.int32),
            jax.ShapeDtypeStruct((ROWS, 128), jnp.float32),
        ),
        in_specs=[SMEM, SMEM, VMEM],
        out_specs=[VMEM] * 2,
        name="prepare",
    )(at, block_len, amax_history)


def quantize_kernel(at_ref, block_ref, scale_ref, pa_ref, rows_ref, one_ref, two_ref, three_ref, pb_ref, up_ref, down_ref, far_ref, q_ref, m_ref, s_ref):
    z, y = at_ref[0], at_ref[1]
    s_ref[0:A] = add(pa_ref[z], rows_ref[0], one_ref[0], three_ref[0], two_ref[0])
    s_ref[A:ROWS] = add(pb_ref[y], up_ref[0], down_ref[0], far_ref[0])
    q_ref[...] = bf(jnp.clip(s_ref[...] * scale_ref[...], -SATURATE, SATURATE))
    size = jnp.abs(s_ref[...])
    block = block_ref[...]
    lane = lax.broadcasted_iota(jnp.int32, (8, 128), 1)
    tops = jnp.zeros((8, 128), jnp.float32)
    for c in range(BLOCKS):
        own = jnp.where(block == c, size, 0.0)
        own = jnp.max(own.reshape(ROWS // 8, 8, 128), axis=0)
        own = jnp.max(jnp.max(own, axis=0, keepdims=True), axis=1, keepdims=True)
        tops = jnp.where(lane == c, own, tops)
    m_ref[...] = jnp.broadcast_to(bf(tops[0:2])[None], (DEVICES, 2, 128))


def quantize(at, *arrays):
    return pl.pallas_call(
        quantize_kernel,
        out_shape=(
            jax.ShapeDtypeStruct((ROWS, 128), jnp.bfloat16),
            jax.ShapeDtypeStruct((DEVICES, 2, 128), jnp.bfloat16),
        ),
        in_specs=[SMEM] + [VMEM] * len(arrays),
        out_specs=[VMEM] * 2,
        scratch_shapes=[pltpu.VMEM((ROWS, 128), jnp.float32)],
        name="quantize",
    )(at, *[in_vmem(a) for a in arrays])


def head(whole, part):
    n = part.shape[0]
    return bf(add(whole, jnp.pad(part, ((0, n), (0, 0), (0, 0)))))


def tail(whole, part):
    n = part.shape[0]
    return bf(add(whole, jnp.pad(part, ((n, 0), (0, 0), (0, 0)))))


def send(x, axis, by, move=shift):
    return move(x, axis, by)


def both_ways(up, down, axis):
    return together(send(up, axis, 1), send(down, axis, -1))


def body(gradients, block_len, amax_history):
    g = gradients.reshape(8, 4, ROWS, 128)
    z, y = lax.axis_index("z"), lax.axis_index("y")

    def for_y(dy, z0=0, nz=8):
        at = (jnp.int32(z0), (y + dy) % 4, jnp.int32(0), jnp.int32(0))
        return lax.dynamic_slice(g, at, (nz, 1, A, 128)).reshape(nz, A, 128)

    def for_z(dz, y0=0, ny=4):
        at = ((z + dz) % 8, jnp.int32(y0), jnp.int32(A), jnp.int32(0))
        return lax.dynamic_slice(g, at, (1, ny, B, 128)).reshape(ny, B, 128)

    b_up, b_dn = both_ways(for_z(4, 0, 2), for_z(4, 2, 2), "z")
    a_up, a_dn = both_ways(for_y(2, 0, 4), for_y(2, 4, 4), "y")
    b_up, b_dn = both_ways(head(for_z(3), b_up), tail(for_z(-3), b_dn), "z")
    a_up, a_dn = both_ways(head(for_y(1), a_up), tail(for_y(-1), a_dn), "y")

    at = jnp.stack([z, y]).astype(jnp.int32)
    block, scale = prepare(at, block_len, amax_history)
    b_up, b_dn, block, scale = together(b_up, b_dn, block, scale)

    b_up, b_dn = both_ways(bf(add(for_z(2), b_up)), bf(add(for_z(-2), b_dn)), "z")
    b_up, b_dn = both_ways(bf(add(for_z(1), b_up)), bf(add(for_z(-1), b_dn)), "z")
    pa = bf(add(for_y(0), a_up, a_dn))

    def chunk(dz):
        return lax.dynamic_slice_in_dim(pa, (z + dz) % 8, 1, 0)

    a_up, a_dn = both_ways(
        jnp.concatenate([chunk(1), chunk(3)]), jnp.concatenate([chunk(-2), chunk(-4)]), "z"
    )
    pb = bf(add(for_z(0), b_up, b_dn))

    def piece(dy):
        return lax.dynamic_slice_in_dim(pb, (y + dy) % 4, 1, 0)

    b_far, b_up, b_dn = send(piece(2), "y", 2), send(piece(1), "y", 1), send(piece(-1), "y", -1)

    a_three = send(bf(add(chunk(-3), a_dn[1:2])), "z", -3)
    a_two = send(bf(add(chunk(2), a_up[1:2])), "z", 2)
    a_one = send(bf(add(chunk(-1), a_dn[0:1])), "z", -1)

    q, m = quantize(at, block, scale, pa, a_up, a_one, a_two, a_three, pb, b_up, b_dn, b_far)

    m = lax.all_to_all(m, ("x", "c", "z", "y"), split_axis=0, concat_axis=0, tiled=True)

    far, near, mirror = send(q, "x", 2, swap), send(q, "x", 1, swap), send(q, "x", 3, swap)
    chips = add(q, far) + add(near, mirror)
    accumulated = chips + send(chips, "c", 1)
    mean_grad = bf(accumulated / scale / DEVICES)
    return mean_grad, jnp.max(m, axis=(0, 1))[:BLOCKS]


def solution(mesh):
    torus = Mesh(mesh.devices.reshape(4, 2, 8, 4), ("x", "c", "z", "y"))
    placed = (P(("x", "c"), ("z", "y"), None, None), P(), P())
    return jax.shard_map(
        body, mesh=torus, in_specs=placed, out_specs=(P(("z", "y"), None), P()), check_vma=False
    )
```

```python
import functools

import jax
import jax.numpy as jnp
from jax import lax
from jax.experimental import pallas as pl
from jax.experimental.pallas import tpu as pltpu
from jax.sharding import Mesh
from jax.sharding import PartitionSpec as P


SATURATE = 448.0
SIZE = {"x": 4, "c": 2, "z": 8, "y": 4}
ROWS = 512
A = 288
B = ROWS - A
BLOCKS = 16
DEVICES = 256


def shift(x, axis, by):
    n = SIZE[axis]
    return lax.ppermute(x, axis, [(i, (i + by) % n) for i in range(n)])


def f32(x):
    return x.astype(jnp.float32)


def add(*terms):
    total = f32(terms[0])
    for t in terms[1:]:
        total = total + f32(t)
    return total


def bf(x):
    return x.astype(jnp.bfloat16)


def together(*arrays):
    return lax.optimization_barrier(arrays)


def swap(x, axis, by):
    return lax.ppermute(x, axis, [(i, i ^ by) for i in range(SIZE[axis])])


def in_vmem(x):
    return pltpu.with_memory_space_constraint(x, pltpu.VMEM)


VMEM = pl.BlockSpec(memory_space=pltpu.VMEM)
SMEM = pl.BlockSpec(memory_space=pltpu.SMEM)
SMALL = pltpu.CompilerParams(vmem_limit_bytes=8 << 20)


def prepare_kernel(at_ref, len_ref, hist_ref, block_ref, scale_ref):
    position = (
        (at_ref[0] * 4 + at_ref[1]) * (ROWS * 128)
        + lax.broadcasted_iota(jnp.int32, (ROWS, 128), 0) * 128
        + lax.broadcasted_iota(jnp.int32, (ROWS, 128), 1)
    )
    largest = jnp.maximum(jnp.max(hist_ref[...], axis=0, keepdims=True), 1.0)
    scales = SATURATE / largest
    block = jnp.zeros((ROWS, 128), jnp.int32)
    scale = jnp.broadcast_to(scales[:, 0:1], (ROWS, 128))
    end = jnp.int32(0)
    for c in range(1, BLOCKS):
        end = end + len_ref[c - 1]
        past = position >= end
        block = jnp.where(past, c, block)
        scale = jnp.where(past, scales[:, c : c + 1], scale)
    block_ref[...] = block
    scale_ref[...] = scale


def prepare(at, block_len, amax_history):
    return pl.pallas_call(
        prepare_kernel,
        out_shape=(
            jax.ShapeDtypeStruct((ROWS, 128), jnp.int32),
            jax.ShapeDtypeStruct((ROWS, 128), jnp.float32),
        ),
        in_specs=[SMEM, SMEM, VMEM],
        out_specs=[VMEM] * 2,
        name="prepare",
        compiler_params=SMALL,
    )(at, block_len, amax_history)


def call(kernel, out, at, *arrays, scratch=()):
    made = pl.pallas_call(
        kernel,
        out_shape=[pltpu.VMEM(shape, jnp.bfloat16) for shape in out],
        in_specs=[SMEM] + [SMEM if a.ndim == 1 else VMEM for a in arrays],
        out_specs=[VMEM] * len(out),
        scratch_shapes=scratch,
        compiler_params=SMALL,
    )(at, *[a if a.ndim == 1 else in_vmem(a) for a in arrays])
    return made


def copied(body, out, at, g):
    return pl.pallas_call(
        body,
        out_shape=[pltpu.VMEM(shape, jnp.bfloat16) for shape in out],
        in_specs=[SMEM, pl.BlockSpec(memory_space=pltpu.HBM)],
        out_specs=[VMEM] * len(out),
        scratch_shapes=[pltpu.SemaphoreType.DMA((8,))],
        compiler_params=SMALL,
    )(at, pltpu.with_memory_space_constraint(g, pltpu.HBM))


def run_copies(sems, pairs):
    copies = [pltpu.make_async_copy(src, dst, sems.at[i]) for i, (src, dst) in enumerate(pairs)]
    for copy in copies:
        copy.start()
    for copy in copies:
        copy.wait()


def open_kernel(at_ref, g_ref, far_z_ref, up_ref, down_ref, sems):
    z, y = at_ref[0], at_ref[1]
    row = (y + 2) % 4
    run_copies(sems, [
        (g_ref.at[(z + 4) % 8, :, A:], far_z_ref),
        (g_ref.at[0:4, row, :A], up_ref),
        (g_ref.at[4:8, row, :A], down_ref),
    ])


def stage_kernel(at_ref, g_ref, out_ref, sems):
    run_copies(sems, [(g_ref.at[i], out_ref.at[i]) for i in range(8)])


def b_first_kernel(at_ref, g_ref, got_ref, up_ref, down_ref):
    z = at_ref[0]
    odd = (z % 2).astype(jnp.float32)
    got = f32(got_ref[...])
    up_ref[...] = bf(f32(g_ref[(z + 3) % 8, :, A:]) + got * odd)
    down_ref[...] = bf(f32(g_ref[(z + 5) % 8, :, A:]) + got * (1.0 - odd))


def b_next_kernel(by, at_ref, g_ref, got_up_ref, got_down_ref, up_ref, down_ref):
    z = at_ref[0]
    up_ref[...] = bf(add(g_ref[(z + by) % 8, :, A:], got_up_ref[...]))
    down_ref[...] = bf(add(g_ref[(z + 8 - by) % 8, :, A:], got_down_ref[...]))


def b_last_kernel(at_ref, g_ref, got_up_ref, got_down_ref, keep_ref, give_ref):
    z, y = at_ref[0], at_ref[1]
    other = y + 1 - 2 * (y % 2)
    for ref, slot, row in ((keep_ref, 0, y), (keep_ref, 1, 3 - y), (give_ref, 0, other), (give_ref, 1, 3 - other)):
        ref[slot] = bf(add(g_ref[z, row, A:], got_up_ref[row], got_down_ref[row]))


def a_first_kernel(at_ref, g_ref, got_up_ref, got_down_ref, up_ref, down_ref):
    y = at_ref[1]
    up, down = (y + 1) % 4, (y + 3) % 4
    up_ref[0:4] = bf(add(g_ref[0:4, up, :A], got_up_ref[...]))
    up_ref[4:8] = g_ref[4:8, up, :A]
    down_ref[0:4] = g_ref[0:4, down, :A]
    down_ref[4:8] = bf(add(g_ref[4:8, down, :A], got_down_ref[...]))


def a_last_kernel(at_ref, g_ref, got_up_ref, got_down_ref, own_ref, up_ref, down_ref, near_ref):
    z, y = at_ref[0], at_ref[1]
    wanted = ((up_ref, 0, 1), (up_ref, 1, 3), (down_ref, 0, 6), (down_ref, 1, 4))
    wanted += ((near_ref, 0, 7), (near_ref, 1, 5), (near_ref, 2, 2), (own_ref, 0, 0))
    for ref, slot, by in wanted:
        row = (z + by) % 8
        ref[slot] = bf(add(g_ref[row, y, :A], got_up_ref[row], got_down_ref[row]))


def quantize_kernel(at_ref, len_ref, block_ref, scale_ref, pa_ref, rows_ref, one_ref, two_ref, three_ref, pb_ref, half_ref, last_ref, q_ref, m_ref, s_ref):
    s_ref[0:A] = add(pa_ref[0], rows_ref[0], one_ref[0], three_ref[0], two_ref[0])
    s_ref[A:ROWS] = add(pb_ref[0], half_ref[0], last_ref[0])
    q_ref[...] = bf(jnp.clip(s_ref[...] * scale_ref[...], -SATURATE, SATURATE))
    start = (at_ref[0] * 4 + at_ref[1]) * (ROWS * 128)
    low, high, end = jnp.int32(0), jnp.int32(0), jnp.int32(0)
    for c in range(BLOCKS - 1):
        end = end + len_ref[c]
        low = low + (start >= end).astype(jnp.int32)
        high = high + (start + (ROWS * 128 - 1) >= end).astype(jnp.int32)
    lane = lax.broadcasted_iota(jnp.int32, (8, 128), 1)

    def one_tensor(c, tops):
        own = jnp.where(block_ref[...] == c, jnp.abs(s_ref[...]), 0.0)
        own = jnp.max(own.reshape(ROWS // 8, 8, 128), axis=0)
        own = jnp.max(jnp.max(own, axis=0, keepdims=True), axis=1, keepdims=True)
        return jnp.where(lane == c, own, tops)

    tops = lax.fori_loop(low, high + 1, one_tensor, jnp.zeros((8, 128), jnp.float32))
    m_ref[...] = jnp.broadcast_to(bf(tops[0:2])[None], m_ref.shape)


def exchange(x, axes):
    return lax.all_to_all(x, axes, split_axis=0, concat_axis=0, tiled=True)


def send(x, axis, by, move=shift):
    return move(x, axis, by)


def both_ways(up, down, axis):
    return send(up, axis, 1), send(down, axis, -1)


def body(gradients, block_len, amax_history):
    g = gradients.reshape(8, 4, ROWS, 128)
    z, y = lax.axis_index("z"), lax.axis_index("y")
    at = jnp.stack([z, y]).astype(jnp.int32)

    four_z, eight_z, four_y = (4, B, 128), (8, A, 128), (2, A, 128)
    got, a_up, a_dn = copied(open_kernel, (four_z, (4, A, 128), (4, A, 128)), at, g)
    got = send(got, "z", 1, swap)
    a_up, a_dn = both_ways(a_up, a_dn, "y")
    (g,) = copied(stage_kernel, ((8, 4, ROWS, 128),), at, g)
    b_up, b_dn = call(b_first_kernel, (four_z, four_z), at, g, got)
    b_up, b_dn = both_ways(b_up, b_dn, "z")
    a_up, a_dn = call(a_first_kernel, (eight_z, eight_z), at, g, a_up, a_dn)
    a_up, a_dn = both_ways(a_up, a_dn, "y")

    block, scale = prepare(at, block_len, amax_history)
    b_up, b_dn, block, scale = together(b_up, b_dn, block, scale)

    b_up, b_dn = call(functools.partial(b_next_kernel, 2), (four_z, four_z), at, g, b_up, b_dn)
    b_up, b_dn = both_ways(b_up, b_dn, "z")
    b_up, b_dn = call(functools.partial(b_next_kernel, 1), (four_z, four_z), at, g, b_up, b_dn)
    b_up, b_dn = both_ways(b_up, b_dn, "z")

    pa, a_up, a_dn, near = call(a_last_kernel, ((1, A, 128), four_y, four_y, (3, A, 128)), at, g, a_up, a_dn)
    a_up, a_dn = both_ways(a_up, a_dn, "z")
    half = (2, B, 128)
    pb, half = call(b_last_kernel, (half, half), at, g, b_up, b_dn)
    half = send(half, "y", 1, swap)

    a_three = send(bf(add(near[1:2], a_dn[1:2])), "z", -3)
    a_two = send(bf(add(near[2:3], a_up[1:2])), "z", 2)
    a_one = send(bf(add(near[0:1], a_dn[0:1])), "z", -1)

    last = send(bf(add(pb[1:2], half[1:2])), "y", 3, swap)

    q, m = call(
        quantize_kernel, ((ROWS, 128), (DEVICES // 2, 2, 128)),
        at, block_len, block, scale, pa, a_up, a_one, a_two, a_three, pb, half, last,
        scratch=[pltpu.VMEM((ROWS, 128), jnp.float32)],
    )

    m = exchange(m, ("x", "z", "y"))

    far, near, mirror = send(q, "x", 2, swap), send(q, "x", 1, swap), send(q, "x", 3, swap)
    chips = add(q, far) + add(near, mirror)
    accumulated = chips + send(chips, "c", 1)
    mean_grad = bf(accumulated / scale / DEVICES)
    m, mean_grad = together(m, mean_grad)
    m = jnp.max(m, axis=0)
    m = jnp.maximum(m, send(m, "c", 1))
    return mean_grad, jnp.max(m, axis=0)[:BLOCKS]


def solution(mesh):
    torus = Mesh(mesh.devices.reshape(4, 2, 8, 4), ("x", "c", "z", "y"))
    placed = (P(("x", "c"), ("z", "y"), None, None), P(), P())
    return jax.shard_map(
        body, mesh=torus, in_specs=placed, out_specs=(P(("z", "y"), None), P()), check_vma=False
    )
```

```python
import functools

import jax
import jax.numpy as jnp
from jax import lax
from jax.experimental import pallas as pl
from jax.experimental.pallas import tpu as pltpu
from jax.sharding import Mesh
from jax.sharding import PartitionSpec as P


SATURATE = 448.0
SIZE = {"x": 4, "c": 2, "z": 8, "y": 4}
ROWS = 512
A = 288
B = ROWS - A
BLOCKS = 16
DEVICES = 256


def shift(x, axis, by):
    n = SIZE[axis]
    return lax.ppermute(x, axis, [(i, (i + by) % n) for i in range(n)])


def f32(x):
    return x.astype(jnp.float32)


def add(*terms):
    total = f32(terms[0])
    for t in terms[1:]:
        total = total + f32(t)
    return total


def bf(x):
    return x.astype(jnp.bfloat16)


def together(*arrays):
    return lax.optimization_barrier(arrays)


def swap(x, axis, by):
    return lax.ppermute(x, axis, [(i, i ^ by) for i in range(SIZE[axis])])


def in_vmem(x):
    return pltpu.with_memory_space_constraint(x, pltpu.VMEM)


VMEM = pl.BlockSpec(memory_space=pltpu.VMEM)
SMEM = pl.BlockSpec(memory_space=pltpu.SMEM)
SMALL = pltpu.CompilerParams(vmem_limit_bytes=8 << 20)


def prepare_kernel(len_ref, hist_ref, block_ref, scale_ref):
    position = (
        (lax.axis_index("z") * 4 + lax.axis_index("y")) * (ROWS * 128)
        + lax.broadcasted_iota(jnp.int32, (ROWS, 128), 0) * 128
        + lax.broadcasted_iota(jnp.int32, (ROWS, 128), 1)
    )
    largest = jnp.maximum(jnp.max(hist_ref[...], axis=0, keepdims=True), 1.0)
    scales = SATURATE / largest
    block = jnp.zeros((ROWS, 128), jnp.int32)
    scale = jnp.broadcast_to(scales[:, 0:1], (ROWS, 128))
    end = jnp.int32(0)
    for c in range(1, BLOCKS):
        end = end + len_ref[c - 1]
        past = position >= end
        block = jnp.where(past, c, block)
        scale = jnp.where(past, scales[:, c : c + 1], scale)
    block_ref[...] = block
    scale_ref[...] = scale


def prepare(block_len, amax_history):
    return pl.pallas_call(
        prepare_kernel,
        out_shape=(
            jax.ShapeDtypeStruct((ROWS, 128), jnp.int32),
            jax.ShapeDtypeStruct((ROWS, 128), jnp.float32),
        ),
        in_specs=[SMEM, VMEM],
        out_specs=[VMEM] * 2,
        name="prepare",
        compiler_params=SMALL,
    )(block_len, amax_history)


def call(kernel, out, *arrays, scratch=()):
    made = pl.pallas_call(
        kernel,
        out_shape=[pltpu.VMEM(shape, jnp.bfloat16) for shape in out],
        in_specs=[VMEM] * len(arrays),
        out_specs=[VMEM] * len(out),
        scratch_shapes=scratch,
        compiler_params=SMALL,
    )(*[in_vmem(a) for a in arrays])
    return made


def copied(body, name, out, g):
    return pl.pallas_call(
        body,
        out_shape=[pltpu.VMEM(shape, jnp.bfloat16) for shape in out],
        in_specs=[pl.BlockSpec(memory_space=pl.ANY if name == "stage" else pltpu.HBM)],
        out_specs=[VMEM] * len(out),
        scratch_shapes=[pltpu.SemaphoreType.DMA((8,))],
        compiler_params=SMALL,
    )(g if name == "stage" else pltpu.with_memory_space_constraint(g, pltpu.HBM))


def run_copies(sems, pairs):
    copies = [pltpu.make_async_copy(src, dst, sems.at[i]) for i, (src, dst) in enumerate(pairs)]
    for copy in copies:
        copy.start()
    for copy in copies:
        copy.wait()


def open_kernel(g_ref, far_z_ref, up_ref, down_ref, sems):
    z, y = lax.axis_index("z"), lax.axis_index("y")
    row = (y + 2) % 4
    run_copies(sems, [
        (g_ref.at[(z + 4) % 8, :, A:], far_z_ref),
        (g_ref.at[0:4, row, :A], up_ref),
        (g_ref.at[4:8, row, :A], down_ref),
    ])


def stage_kernel(g_ref, out_ref, sems):
    run_copies(sems, [(g_ref.at[i], out_ref.at[i]) for i in range(8)])


def b_first_kernel(g_ref, got_ref, up_ref, down_ref):
    z = lax.axis_index("z")
    odd = (z % 2).astype(jnp.float32)
    got = f32(got_ref[...])
    up_ref[...] = bf(f32(g_ref[(z + 3) % 8, :, A:]) + got * odd)
    down_ref[...] = bf(f32(g_ref[(z + 5) % 8, :, A:]) + got * (1.0 - odd))


def b_next_kernel(by, g_ref, got_up_ref, got_down_ref, up_ref, down_ref):
    z = lax.axis_index("z")
    up_ref[...] = bf(add(g_ref[(z + by) % 8, :, A:], got_up_ref[...]))
    down_ref[...] = bf(add(g_ref[(z + 8 - by) % 8, :, A:], got_down_ref[...]))


def b_last_kernel(g_ref, got_up_ref, got_down_ref, keep_ref, give_ref):
    z, y = lax.axis_index("z"), lax.axis_index("y")
    other = y + 1 - 2 * (y % 2)
    for ref, slot, row in ((keep_ref, 0, y), (keep_ref, 1, 3 - y), (give_ref, 0, other), (give_ref, 1, 3 - other)):
        ref[slot] = bf(add(g_ref[z, row, A:], got_up_ref[row], got_down_ref[row]))


def a_first_kernel(g_ref, got_up_ref, got_down_ref, up_ref, down_ref):
    y = lax.axis_index("y")
    up, down = (y + 1) % 4, (y + 3) % 4
    up_ref[0:4] = bf(add(g_ref[0:4, up, :A], got_up_ref[...]))
    up_ref[4:8] = g_ref[4:8, up, :A]
    down_ref[0:4] = g_ref[0:4, down, :A]
    down_ref[4:8] = bf(add(g_ref[4:8, down, :A], got_down_ref[...]))


def a_last_kernel(g_ref, got_up_ref, got_down_ref, own_ref, up_ref, down_ref, near_ref):
    z, y = lax.axis_index("z"), lax.axis_index("y")
    wanted = ((up_ref, 0, 1), (up_ref, 1, 3), (down_ref, 0, 6), (down_ref, 1, 4))
    wanted += ((near_ref, 0, 7), (near_ref, 1, 5), (near_ref, 2, 2), (own_ref, 0, 0))
    for ref, slot, by in wanted:
        row = (z + by) % 8
        ref[slot] = bf(add(g_ref[row, y, :A], got_up_ref[row], got_down_ref[row]))


def quantize_kernel(block_ref, scale_ref, pa_ref, rows_ref, one_ref, two_ref, three_ref, pb_ref, half_ref, last_ref, q_ref, m_ref, s_ref):
    s_ref[0:A] = add(pa_ref[0], rows_ref[0], one_ref[0], three_ref[0], two_ref[0])
    s_ref[A:ROWS] = add(pb_ref[0], half_ref[0], last_ref[0])
    q_ref[...] = bf(jnp.clip(s_ref[...] * scale_ref[...], -SATURATE, SATURATE))
    low, high = block_ref[0, 0], block_ref[ROWS - 1, 127]
    lane = lax.broadcasted_iota(jnp.int32, (8, 128), 1)

    def one_tensor(c, tops):
        own = jnp.where(block_ref[...] == c, jnp.abs(s_ref[...]), 0.0)
        own = jnp.max(own.reshape(ROWS // 8, 8, 128), axis=0)
        own = jnp.max(jnp.max(own, axis=0, keepdims=True), axis=1, keepdims=True)
        return jnp.where(lane == c, own, tops)

    tops = lax.fori_loop(low, high + 1, one_tensor, jnp.zeros((8, 128), jnp.float32))
    m_ref[...] = jnp.broadcast_to(bf(tops[0:2])[None], m_ref.shape)


def exchange(x, axes):
    return lax.all_to_all(x, axes, split_axis=0, concat_axis=0, tiled=True)


def send(x, axis, by, move=shift):
    return move(x, axis, by)


def both_ways(up, down, axis):
    return send(up, axis, 1), send(down, axis, -1)


def body(gradients, block_len, amax_history):
    g = gradients.reshape(8, 4, ROWS, 128)
    four_z, eight_z, four_y = (4, B, 128), (8, A, 128), (2, A, 128)
    got, a_up, a_dn = copied(open_kernel, "open", (four_z, (4, A, 128), (4, A, 128)), g)
    got = send(got, "z", 1, swap)
    a_up, a_dn = both_ways(a_up, a_dn, "y")
    (g,) = copied(stage_kernel, "stage", ((8, 4, ROWS, 128),), g)
    b_up, b_dn = call(b_first_kernel, (four_z, four_z), g, got)
    b_up, b_dn = both_ways(b_up, b_dn, "z")
    a_up, a_dn = call(a_first_kernel, (eight_z, eight_z), g, a_up, a_dn)
    a_up, a_dn = both_ways(a_up, a_dn, "y")

    b_up, b_dn = call(functools.partial(b_next_kernel, 2), (four_z, four_z), g, b_up, b_dn)
    b_up, b_dn, block_len = together(b_up, b_dn, block_len)
    b_up, b_dn = both_ways(b_up, b_dn, "z")
    block, scale = prepare(block_len, amax_history)
    b_up, b_dn, block, scale = together(b_up, b_dn, block, scale)
    b_up, b_dn = call(functools.partial(b_next_kernel, 1), (four_z, four_z), g, b_up, b_dn)
    b_up, b_dn = both_ways(b_up, b_dn, "z")

    pa, a_up, a_dn, near = call(a_last_kernel, ((1, A, 128), four_y, four_y, (3, A, 128)), g, a_up, a_dn)
    a_up, a_dn = both_ways(a_up, a_dn, "z")
    half = (2, B, 128)
    pb, half = call(b_last_kernel, (half, half), g, b_up, b_dn)
    half = send(half, "y", 1, swap)

    a_three = send(bf(add(near[1:2], a_dn[1:2])), "z", -3)
    a_two = send(bf(add(near[2:3], a_up[1:2])), "z", 2)
    a_one = send(bf(add(near[0:1], a_dn[0:1])), "z", -1)

    last = send(bf(add(pb[1:2], half[1:2])), "y", 3, swap)

    q, m = call(
        quantize_kernel, ((ROWS, 128), (DEVICES // 2, 2, 128)),
        block, scale, pa, a_up, a_one, a_two, a_three, pb, half, last,
        scratch=[pltpu.VMEM((ROWS, 128), jnp.float32)],
    )

    m = exchange(m, ("x", "z", "y"))

    far, near, mirror = send(q, "x", 2, swap), send(q, "x", 1, swap), send(q, "x", 3, swap)
    chips = add(q, far) + add(near, mirror)
    accumulated = chips + send(chips, "c", 1)
    mean_grad = bf(accumulated / scale / DEVICES)
    m, mean_grad = together(m, mean_grad)
    m = jnp.max(m, axis=0)
    m = jnp.maximum(m, send(m, "c", 1))
    return mean_grad, jnp.max(m, axis=0)[:BLOCKS]


def solution(mesh):
    torus = Mesh(mesh.devices.reshape(4, 2, 8, 4), ("x", "c", "z", "y"))
    placed = (P(("x", "c"), ("z", "y"), None, None), P(), P())
    return jax.shard_map(
        body, mesh=torus, in_specs=placed, out_specs=(P(("z", "y"), None), P()), check_vma=False
    )
```

```python
import functools

import jax
import jax.numpy as jnp
from jax import lax
from jax.experimental import pallas as pl
from jax.experimental.pallas import tpu as pltpu
from jax.sharding import Mesh
from jax.sharding import PartitionSpec as P


SATURATE = 448.0
SIZE = {"x": 4, "c": 2, "z": 8, "y": 4}
ROWS = 512
A = 288
B = ROWS - A
BLOCKS = 16
DEVICES = 256


def shift(x, axis, by):
    n = SIZE[axis]
    return lax.ppermute(x, axis, [(i, (i + by) % n) for i in range(n)])


def f32(x):
    return x.astype(jnp.float32)


def add(*terms):
    total = f32(terms[0])
    for t in terms[1:]:
        total = total + f32(t)
    return total


def bf(x):
    return x.astype(jnp.bfloat16)


def together(*arrays):
    return lax.optimization_barrier(arrays)


def swap(x, axis, by):
    return lax.ppermute(x, axis, [(i, i ^ by) for i in range(SIZE[axis])])


def in_vmem(x):
    return pltpu.with_memory_space_constraint(x, pltpu.VMEM)


VMEM = pl.BlockSpec(memory_space=pltpu.VMEM)
SMEM = pl.BlockSpec(memory_space=pltpu.SMEM)
SMALL = pltpu.CompilerParams(vmem_limit_bytes=8 << 20)


def prepare_kernel(len_ref, hist_ref, block_ref, scale_ref):
    position = (
        (lax.axis_index("z") * 4 + lax.axis_index("y")) * (ROWS * 128)
        + lax.broadcasted_iota(jnp.int32, (ROWS, 128), 0) * 128
        + lax.broadcasted_iota(jnp.int32, (ROWS, 128), 1)
    )
    largest = jnp.maximum(jnp.max(hist_ref[...], axis=0, keepdims=True), 1.0)
    scales = SATURATE / largest
    block = jnp.zeros((ROWS, 128), jnp.int32)
    scale = jnp.broadcast_to(scales[:, 0:1], (ROWS, 128))
    end = jnp.int32(0)
    for c in range(1, BLOCKS):
        end = end + len_ref[c - 1]
        past = position >= end
        block = jnp.where(past, c, block)
        scale = jnp.where(past, scales[:, c : c + 1], scale)
    block_ref[...] = block
    scale_ref[...] = scale


def prepare(block_len, amax_history):
    return pl.pallas_call(
        prepare_kernel,
        out_shape=(
            jax.ShapeDtypeStruct((ROWS, 128), jnp.int32),
            jax.ShapeDtypeStruct((ROWS, 128), jnp.float32),
        ),
        in_specs=[SMEM, VMEM],
        out_specs=[VMEM] * 2,
        name="prepare",
        compiler_params=SMALL,
    )(block_len, amax_history)


def call(kernel, out, *arrays, scratch=()):
    made = pl.pallas_call(
        kernel,
        out_shape=[pltpu.VMEM(shape, jnp.bfloat16) for shape in out],
        in_specs=[VMEM] * len(arrays),
        out_specs=[VMEM] * len(out),
        scratch_shapes=scratch,
        compiler_params=SMALL,
    )(*[in_vmem(a) for a in arrays])
    return made


def copied(body, name, out, g):
    return pl.pallas_call(
        body,
        out_shape=[pltpu.VMEM(shape, jnp.bfloat16) for shape in out],
        in_specs=[pl.BlockSpec(memory_space=pl.ANY if name == "stage" else pltpu.HBM)],
        out_specs=[VMEM] * len(out),
        scratch_shapes=[pltpu.SemaphoreType.DMA((12,))],
        compiler_params=SMALL,
    )(g if name == "stage" else pltpu.with_memory_space_constraint(g, pltpu.HBM))


def run_copies(sems, pairs):
    copies = [pltpu.make_async_copy(src, dst, sems.at[i]) for i, (src, dst) in enumerate(pairs)]
    for copy in copies:
        copy.start()
    for copy in copies:
        copy.wait()


def open_kernel(g_ref, far_z_ref, up_ref, down_ref, sems):
    z, y = lax.axis_index("z"), lax.axis_index("y")
    row = (y + 2) % 4
    run_copies(sems, [
        *[(g_ref.at[(z + 4) % 8, i, A:], far_z_ref.at[i]) for i in range(4)],
        *[(g_ref.at[i, row, :A], up_ref.at[i]) for i in range(4)],
        *[(g_ref.at[4 + i, row, :A], down_ref.at[i]) for i in range(4)],
    ])


def stage_kernel(g_ref, out_ref, sems):
    run_copies(sems, [(g_ref.at[i], out_ref.at[i]) for i in range(8)])


def b_first_kernel(g_ref, got_ref, up_ref, down_ref):
    z = lax.axis_index("z")
    odd = (z % 2).astype(jnp.float32)
    got = f32(got_ref[...])
    up_ref[...] = bf(f32(g_ref[(z + 3) % 8, :, A:]) + got * odd)
    down_ref[...] = bf(f32(g_ref[(z + 5) % 8, :, A:]) + got * (1.0 - odd))


def b_next_kernel(by, g_ref, got_up_ref, got_down_ref, up_ref, down_ref):
    z = lax.axis_index("z")
    up_ref[...] = bf(add(g_ref[(z + by) % 8, :, A:], got_up_ref[...]))
    down_ref[...] = bf(add(g_ref[(z + 8 - by) % 8, :, A:], got_down_ref[...]))


def b_last_kernel(g_ref, got_up_ref, got_down_ref, keep_ref, give_ref):
    z, y = lax.axis_index("z"), lax.axis_index("y")
    other = y + 1 - 2 * (y % 2)
    for ref, slot, row in ((keep_ref, 0, y), (keep_ref, 1, 3 - y), (give_ref, 0, other), (give_ref, 1, 3 - other)):
        ref[slot] = bf(add(g_ref[z, row, A:], got_up_ref[row], got_down_ref[row]))


def a_first_kernel(g_ref, got_up_ref, got_down_ref, up_ref, down_ref):
    y = lax.axis_index("y")
    up, down = (y + 1) % 4, (y + 3) % 4
    up_ref[0:4] = bf(add(g_ref[0:4, up, :A], got_up_ref[...]))
    up_ref[4:8] = g_ref[4:8, up, :A]
    down_ref[0:4] = g_ref[0:4, down, :A]
    down_ref[4:8] = bf(add(g_ref[4:8, down, :A], got_down_ref[...]))


def a_last_kernel(g_ref, got_up_ref, got_down_ref, own_ref, up_ref, down_ref, near_ref):
    z, y = lax.axis_index("z"), lax.axis_index("y")
    wanted = ((up_ref, 0, 1), (up_ref, 1, 3), (down_ref, 0, 6), (down_ref, 1, 4))
    wanted += ((near_ref, 0, 7), (near_ref, 1, 5), (near_ref, 2, 2), (own_ref, 0, 0))
    for ref, slot, by in wanted:
        row = (z + by) % 8
        ref[slot] = bf(add(g_ref[row, y, :A], got_up_ref[row], got_down_ref[row]))


def quantize_kernel(block_ref, scale_ref, pa_ref, rows_ref, one_ref, two_ref, three_ref, pb_ref, half_ref, last_ref, q_ref, m_ref, s_ref):
    s_ref[0:A] = add(pa_ref[0], rows_ref[0], one_ref[0], three_ref[0], two_ref[0])
    s_ref[A:ROWS] = add(pb_ref[0], half_ref[0], last_ref[0])
    q_ref[...] = bf(jnp.clip(s_ref[...] * scale_ref[...], -SATURATE, SATURATE))
    low, high = block_ref[0, 0], block_ref[ROWS - 1, 127]
    lane = lax.broadcasted_iota(jnp.int32, (8, 128), 1)

    def one_tensor(c, tops):
        own = jnp.where(block_ref[...] == c, jnp.abs(s_ref[...]), 0.0)
        own = jnp.max(own.reshape(ROWS // 8, 8, 128), axis=0)
        own = jnp.max(jnp.max(own, axis=0, keepdims=True), axis=1, keepdims=True)
        return jnp.where(lane == c, own, tops)

    tops = lax.fori_loop(low, high + 1, one_tensor, jnp.zeros((8, 128), jnp.float32))
    m_ref[...] = jnp.broadcast_to(bf(tops[0:2])[None], m_ref.shape)


def exchange(x, axes):
    return lax.all_to_all(x, axes, split_axis=0, concat_axis=0, tiled=True)


def send(x, axis, by, move=shift):
    return move(x, axis, by)


def both_ways(up, down, axis):
    return send(up, axis, 1), send(down, axis, -1)


def body(gradients, block_len, amax_history):
    g = gradients.reshape(8, 4, ROWS, 128)
    four_z, eight_z, four_y = (4, B, 128), (8, A, 128), (2, A, 128)
    got, a_up, a_dn = copied(open_kernel, "open", (four_z, (4, A, 128), (4, A, 128)), g)
    got = send(got, "z", 1, swap)
    a_up, a_dn = both_ways(a_up, a_dn, "y")
    (g,) = copied(stage_kernel, "stage", ((8, 4, ROWS, 128),), g)
    b_up, b_dn = call(b_first_kernel, (four_z, four_z), g, got)
    b_up, b_dn = both_ways(b_up, b_dn, "z")
    a_up, a_dn = call(a_first_kernel, (eight_z, eight_z), g, a_up, a_dn)
    a_up, a_dn = both_ways(a_up, a_dn, "y")

    b_up, b_dn = call(functools.partial(b_next_kernel, 2), (four_z, four_z), g, b_up, b_dn)
    b_up, b_dn, block_len = together(b_up, b_dn, block_len)
    b_up, b_dn = both_ways(b_up, b_dn, "z")
    block, scale = prepare(block_len, amax_history)
    b_up, b_dn, block, scale = together(b_up, b_dn, block, scale)
    b_up, b_dn = call(functools.partial(b_next_kernel, 1), (four_z, four_z), g, b_up, b_dn)
    b_up, b_dn = both_ways(b_up, b_dn, "z")

    pa, a_up, a_dn, near = call(a_last_kernel, ((1, A, 128), four_y, four_y, (3, A, 128)), g, a_up, a_dn)
    a_up, a_dn = both_ways(a_up, a_dn, "z")
    half = (2, B, 128)
    pb, half = call(b_last_kernel, (half, half), g, b_up, b_dn)
    half = send(half, "y", 1, swap)

    a_three = send(bf(add(near[1:2], a_dn[1:2])), "z", -3)
    a_two = send(bf(add(near[2:3], a_up[1:2])), "z", 2)
    a_one = send(bf(add(near[0:1], a_dn[0:1])), "z", -1)

    last = send(bf(add(pb[1:2], half[1:2])), "y", 3, swap)

    q, m = call(
        quantize_kernel, ((ROWS, 128), (DEVICES, 2, 128)),
        block, scale, pa, a_up, a_one, a_two, a_three, pb, half, last,
        scratch=[pltpu.VMEM((ROWS, 128), jnp.float32)],
    )

    m = exchange(m, ("x", "c", "z", "y"))

    far, near, mirror = send(q, "x", 2, swap), send(q, "x", 1, swap), send(q, "x", 3, swap)
    chips = add(q, far) + add(near, mirror)
    accumulated = chips + send(chips, "c", 1)
    mean_grad = bf(accumulated / scale / DEVICES)
    m = jnp.max(m, axis=0)
    return mean_grad, jnp.max(m, axis=0)[:BLOCKS]


def solution(mesh):
    torus = Mesh(mesh.devices.reshape(4, 2, 8, 4), ("x", "c", "z", "y"))
    placed = (P(("x", "c"), ("z", "y"), None, None), P(), P())
    return jax.shard_map(
        body, mesh=torus, in_specs=placed, out_specs=(P(("z", "y"), None), P()), check_vma=False
    )
```
